8 devices in a mesh: part: 1 (over z), tpa: 2 (over y), tpb: 4 (over x, core).
Axes of the slice: x: 2, y: 2, z: 1, core: 2. Of those that a mesh axis runs over, the one named last changes fastest.
Arguments:
- x: bfloat16 [64, 512, 2048], P(('part', 'tpb'))
- lengths: int32 [64], P(('part', 'tpb'))
- k_buf: bfloat16 [64, 512, 32, 64], P(('part', 'tpb'), None, 'tpa')
- v_buf: bfloat16 [64, 512, 32, 64], P(('part', 'tpb'), None, 'tpa')
- w_qkv: bfloat16 [2048, 6144], P('part', ('tpa', 'tpb'))
- w_o: bfloat16 [2048, 2048], P(('part', 'tpa', 'tpb'))
- w_gate_up: bfloat16 [2048, 16384], P('part', ('tpa', 'tpb'))
- w_down: bfloat16 [8192, 2048], P(('part', 'tpa', 'tpb'))
- g_attn: bfloat16 [2048], P('part')
- g_mlp: bfloat16 [2048], P('part')
Outputs:
- output 1: bfloat16 [64, 512, 2048], P(('part', 'tpb'))
- output 2: bfloat16 [64, 512, 32, 64], P(('part', 'tpb'), None, 'tpa')
- output 3: bfloat16 [64, 512, 32, 64], P(('part', 'tpb'), None, 'tpa')
- output 4: bfloat16 [2048, 2048], P('part', 'tpa')
- output 5: bfloat16 [2048, 2048], P('part', 'tpa')
- output 6: bfloat16 [2048, 2048], P('part', 'tpa')
- output 7: bfloat16 [2048, 2048], P(('part', 'tpa'))
- output 8: bfloat16 [2048, 8192], P('part', 'tpa')
- output 9: bfloat16 [2048, 8192], P('part', 'tpa')
- output 10: bfloat16 [8192, 2048], P(('part', 'tpa'))
All inputs are finite; a program needn't handle non-finite values.
Results may differ from the reference program's by a relative error of at most 0.0129807.
Values are sent between devices in bfloat16 or wider.
A program may use at most 1 GiB of HBM per device.

```python
import math
import jax
import jax.numpy as jnp
from jax import lax

D = 2048
HEADS = 32
KV_HEADS = 32
HEAD = 64
FF = 8192
BATCH = 64
SEQ = 512
TRAIN_TP = 8
GROUP = HEADS // KV_HEADS
QKV_COLS = KV_HEADS * (GROUP + 2) * HEAD
FF_BLOCK = FF // TRAIN_TP
ROPE_BASE = 500000.0
ROPE_FACTOR = 8.0
LOW_FREQ = 1.0
HIGH_FREQ = 4.0
ORIG_CONTEXT = 8192.0
NORM_EPS = 1e-5
MASK_VALUE = -1e30


def setup_inputs(seed: int = 0, part: int = 0) -> dict:
    part_key = jax.random.fold_in(jax.random.key(seed), part)
    sub_keys = jax.random.split(part_key, 10)
    x_in = jax.random.normal(sub_keys[0], (BATCH, SEQ, D), jnp.float32)
    drawn_len = jax.random.randint(sub_keys[1], (BATCH,), 1, SEQ + 1)
    lengths = jnp.where(jnp.arange(BATCH) == 0, SEQ, drawn_len).astype(jnp.int32)
    k_buf = jax.random.normal(sub_keys[2], (BATCH, SEQ, KV_HEADS, HEAD), jnp.float32)
    v_buf = jax.random.normal(sub_keys[3], (BATCH, SEQ, KV_HEADS, HEAD), jnp.float32)
    qk_scale = jnp.where(jnp.arange(GROUP + 2) <= GROUP, 1.5, 1.0)[:, None]
    w_qkv = (jax.random.normal(sub_keys[4], (D, KV_HEADS, GROUP + 2, HEAD), jnp.float32) * qk_scale * D ** -0.5).reshape(D, QKV_COLS)
    w_o = jax.random.normal(sub_keys[5], (HEADS * HEAD, D), jnp.float32) * (HEADS * HEAD) ** -0.5
    w_gate_up = jax.random.normal(sub_keys[6], (D, 2 * FF), jnp.float32) * D ** -0.5
    w_down = jax.random.normal(sub_keys[7], (FF, D), jnp.float32) * FF ** -0.5
    g_attn = 1.0 + 0.4 * jax.random.normal(sub_keys[8], (D,), jnp.float32)
    g_mlp = 1.0 + 0.4 * jax.random.normal(sub_keys[9], (D,), jnp.float32)
    return {'x': x_in.astype(jnp.bfloat16), 'lengths': lengths, 'k_buf': k_buf.astype(jnp.bfloat16), 'v_buf': v_buf.astype(jnp.bfloat16), 'w_qkv': w_qkv.astype(jnp.bfloat16), 'w_o': w_o.astype(jnp.bfloat16), 'w_gate_up': w_gate_up.astype(jnp.bfloat16), 'w_down': w_down.astype(jnp.bfloat16), 'g_attn': g_attn.astype(jnp.bfloat16), 'g_mlp': g_mlp.astype(jnp.bfloat16)}


def rms_norm(x_in, gain_vec):
    x_wide = x_in.astype(jnp.float32)
    mean_sq = jnp.mean(x_wide * x_wide, axis=-1, keepdims=True)
    return (x_wide * lax.rsqrt(mean_sq + NORM_EPS) * gain_vec.astype(jnp.float32)).astype(jnp.bfloat16)


def rope_tables():
    exponent = jnp.arange(HEAD // 2, dtype=jnp.float32) * (2.0 / HEAD)
    inv_freq = 1.0 / jnp.power(ROPE_BASE, exponent)
    wavelen = 2.0 * math.pi / inv_freq
    smooth = (ORIG_CONTEXT / wavelen - LOW_FREQ) / (HIGH_FREQ - LOW_FREQ)
    blended = (1.0 - smooth) * inv_freq / ROPE_FACTOR + smooth * inv_freq
    rope_freq = jnp.where(wavelen < ORIG_CONTEXT / HIGH_FREQ, inv_freq, jnp.where(wavelen > ORIG_CONTEXT / LOW_FREQ, inv_freq / ROPE_FACTOR, blended))
    angles = jnp.arange(SEQ, dtype=jnp.float32)[:, None] * rope_freq[None, :]
    return jnp.cos(angles), jnp.sin(angles)


def apply_rope(vec_in, cos_tab, sin_tab):
    half_dim = vec_in.shape[-1] // 2
    first_half = vec_in[..., :half_dim]
    second_half = vec_in[..., half_dim:]
    return jnp.concatenate([first_half * cos_tab - second_half * sin_tab, second_half * cos_tab + first_half * sin_tab], axis=-1)


def reference(x, lengths, k_buf, v_buf, w_qkv, w_o, w_gate_up, w_down, g_attn, g_mlp):
    packed = w_qkv.reshape(D, KV_HEADS, GROUP + 2, HEAD)
    w_q = packed[:, :, :GROUP, :].reshape(D, HEADS * HEAD)
    w_k = packed[:, :, GROUP, :].reshape(D, KV_HEADS * HEAD)
    w_v = packed[:, :, GROUP + 1, :].reshape(D, KV_HEADS * HEAD)
    gu_view = w_gate_up.reshape(D, TRAIN_TP, 2, FF_BLOCK)
    w_gate = gu_view[:, :, 0, :].reshape(D, FF)
    w_up = gu_view[:, :, 1, :].reshape(D, FF)
    cos_tab, sin_tab = rope_tables()
    positions = jnp.arange(SEQ)
    causal = positions[None, :] <= positions[:, None]

    def one_prompt(prompt_item):
        tokens, length = prompt_item
        x_normed = rms_norm(tokens, g_attn)
        queries = jnp.dot(x_normed, w_q, preferred_element_type=jnp.float32).astype(jnp.bfloat16).reshape(SEQ, KV_HEADS, GROUP, HEAD)
        keys_new = jnp.dot(x_normed, w_k, preferred_element_type=jnp.float32).astype(jnp.bfloat16).reshape(SEQ, KV_HEADS, HEAD)
        values = jnp.dot(x_normed, w_v, preferred_element_type=jnp.float32).astype(jnp.bfloat16).reshape(SEQ, KV_HEADS, HEAD)
        q_rot = apply_rope(queries.astype(jnp.float32), cos_tab[:, None, None, :], sin_tab[:, None, None, :]).astype(jnp.bfloat16)
        k_rot = apply_rope(keys_new.astype(jnp.float32), cos_tab[:, None, :], sin_tab[:, None, :]).astype(jnp.bfloat16)
        allowed = causal & (positions[None, :] < length)

        def one_group(kv_item):
            q_head, k_head, v_head = kv_item
            scores = jnp.einsum('qgd,sd->gqs', q_head.astype(jnp.float32), k_head.astype(jnp.float32)) * HEAD ** -0.5
            scores = jnp.where(allowed[None], scores, MASK_VALUE)
            attn_prob = jax.nn.softmax(scores, axis=-1).astype(jnp.bfloat16)
            return jnp.einsum('gqs,sd->qgd', attn_prob.astype(jnp.float32), v_head.astype(jnp.float32)).astype(jnp.bfloat16)

        per_group = lax.map(one_group, (q_rot.transpose(1, 0, 2, 3), k_rot.transpose(1, 0, 2), values.transpose(1, 0, 2)))
        attn_out = per_group.transpose(1, 0, 2, 3).reshape(SEQ, HEADS * HEAD)
        attn_proj = jnp.dot(attn_out, w_o, preferred_element_type=jnp.float32)
        hidden = (tokens.astype(jnp.float32) + attn_proj).astype(jnp.bfloat16)
        h_normed = rms_norm(hidden, g_mlp)
        gate_act = jnp.dot(h_normed, w_gate, preferred_element_type=jnp.float32).astype(jnp.bfloat16)
        up_act = jnp.dot(h_normed, w_up, preferred_element_type=jnp.float32).astype(jnp.bfloat16)
        mid_act = (jax.nn.silu(gate_act.astype(jnp.float32)) * up_act.astype(jnp.float32)).astype(jnp.bfloat16)
        layer_out = (hidden.astype(jnp.float32) + jnp.dot(mid_act, w_down, preferred_element_type=jnp.float32)).astype(jnp.bfloat16)
        return layer_out, k_rot, values

    layer_out, k_new, v_new = lax.map(one_prompt, (x, lengths))
    valid_pos = (positions[None, :] < lengths[:, None])[:, :, None, None]
    k_cache = jnp.where(valid_pos, k_new, k_buf)
    v_cache = jnp.where(valid_pos, v_new, v_buf)
    return (layer_out, k_cache, v_cache, w_q, w_k, w_v, w_o, w_gate, w_up, w_down)
```

```python
import functools
import math
import jax
import jax.numpy as jnp
from jax import lax
from jax.experimental import pallas as pl
from jax.experimental.layout import Layout, with_layout_constraint
from jax.experimental.pallas import tpu as pltpu
from jax.sharding import PartitionSpec as P

ROPE_BASE = 500000.0
ROPE_FACTOR = 8.0
LOW_FREQ = 1.0
HIGH_FREQ = 4.0
ORIG_CONTEXT = 8192.0
NORM_EPS = 1e-5
MASK_VALUE = -1e30
BF16 = jnp.bfloat16
F32 = jnp.float32
SHARED = 0
CHUNK = 2


def rms_norm(x_in, gain_vec):
    x_wide = x_in.astype(F32)
    mean_sq = jnp.mean(x_wide * x_wide, axis=-1, keepdims=True)
    return (x_wide * lax.rsqrt(mean_sq + NORM_EPS) * gain_vec.astype(F32)).astype(BF16)


def rope_angles(seq_len, head_dim):
    exponent = jnp.arange(head_dim // 2, dtype=F32) * (2.0 / head_dim)
    inv_freq = 1.0 / jnp.power(ROPE_BASE, exponent)
    wavelen = 2.0 * math.pi / inv_freq
    smooth = (ORIG_CONTEXT / wavelen - LOW_FREQ) / (HIGH_FREQ - LOW_FREQ)
    blended = (1.0 - smooth) * inv_freq / ROPE_FACTOR + smooth * inv_freq
    freq = jnp.where(wavelen < ORIG_CONTEXT / HIGH_FREQ, inv_freq, jnp.where(wavelen > ORIG_CONTEXT / LOW_FREQ, inv_freq / ROPE_FACTOR, blended))
    return jnp.arange(seq_len, dtype=F32)[:, None] * freq[None, :]


def matmul(lhs, rhs):
    return jnp.einsum('bsd,dc->bsc', lhs, rhs, preferred_element_type=F32)


def matmul_t(lhs, rhs):
    prod = with_layout_constraint(matmul(lhs, rhs), Layout((0, 2, 1)))
    return jnp.transpose(prod, (0, 2, 1)).astype(BF16)


def rope_rows(first, second, cos_t, sin_t):
    return first * cos_t - second * sin_t, second * cos_t + first * sin_t


def attn_kernel(len_ref, q_ref, k_ref, v_ref, cos_ref, sin_ref, cos_t_ref, sin_t_ref, o_ref, *, half, blk):
    seq = q_ref.shape[1]
    hd = 2 * half
    length = len_ref[pl.program_id(0)]
    cos_t, sin_t = cos_t_ref[...], sin_t_ref[...]
    keys = []
    for h in range(2):
        k_first = k_ref[0, h * hd:h * hd + half, :].astype(F32)
        k_second = k_ref[0, h * hd + half:(h + 1) * hd, :].astype(F32)
        lo, hi = rope_rows(k_first, k_second, cos_t, sin_t)
        keys.append(jnp.concatenate([lo, hi], axis=0).astype(BF16))
    for i in range(seq // blk):
        rows = slice(i * blk, (i + 1) * blk)
        width = (i + 1) * blk
        q_in = q_ref[0, rows, :].astype(F32)
        lane = lax.broadcasted_iota(jnp.int32, q_in.shape, 1)
        swapped = jnp.where(lane % hd < half, pltpu.roll(q_in, 2 * hd - half, 1), pltpu.roll(q_in, half, 1))
        q_rot = (q_in * cos_ref[rows, :] + swapped * sin_ref[rows, :]).astype(BF16) * BF16(hd ** -0.5)
        row = lax.broadcasted_iota(jnp.int32, (blk, width), 0) + i * blk
        col = lax.broadcasted_iota(jnp.int32, (blk, width), 1)
        allowed = col <= jnp.minimum(row, length - 1)
        outs = []
        for h in range(2):
            scores = jnp.dot(q_rot[:, h * hd:(h + 1) * hd], keys[h][:, :width], preferred_element_type=F32)
            scores = jnp.where(allowed, scores, MASK_VALUE)
            expd = jnp.exp(scores - jnp.max(scores, axis=-1, keepdims=True))
            prob = (expd * (1.0 / jnp.sum(expd, axis=-1, keepdims=True))).astype(BF16)
            outs.append(lax.dot_general(prob, v_ref[0, :, :width], (((1,), (1,)), ((), ())), preferred_element_type=F32))
        o_ref[0, rows, :] = jnp.where(lane < hd, outs[0], outs[1]).astype(BF16)


def attention(lengths, q, k_t, v_t, angles):
    batch, seq, width = q.shape
    half = angles.shape[1]
    hd = 2 * half
    cos, sin = jnp.cos(angles), jnp.sin(angles)
    cos_row = jnp.tile(jnp.concatenate([cos, cos], axis=1), (1, 2))
    sin_row = jnp.tile(jnp.concatenate([-sin, sin], axis=1), (1, 2))
    whole = lambda shape: pl.BlockSpec(shape, lambda b, j, *_: (0, 0))
    return pl.pallas_call(
        functools.partial(attn_kernel, half=half, blk=256),
        grid_spec=pltpu.PrefetchScalarGridSpec(
            num_scalar_prefetch=1,
            grid=(batch, width // (2 * hd)),
            in_specs=[
                pl.BlockSpec((1, seq, 2 * hd), lambda b, j, *_: (b, 0, j)),
                pl.BlockSpec((1, 2 * hd, seq), lambda b, j, *_: (b, j, 0)),
                pl.BlockSpec((1, 2 * hd, seq), lambda b, j, *_: (b, j, 0)),
                whole((seq, 2 * hd)), whole((seq, 2 * hd)), whole((half, seq)), whole((half, seq)),
            ],
            out_specs=pl.BlockSpec((1, seq, 2 * hd), lambda b, j, *_: (b, 0, j)),
        ),
        out_shape=jax.ShapeDtypeStruct(q.shape, BF16),
        compiler_params=pltpu.CompilerParams(dimension_semantics=("parallel", "arbitrary")),
        cost_estimate=pl.CostEstimate(flops=batch * width * seq * seq * 16, bytes_accessed=8 * q.size, transcendentals=0),
        name="prefill_attention",
    )(lengths, q, k_t, v_t, cos_row, sin_row, cos.T, sin.T)


def cache_kernel(pos_ref, len_ref, k_own, v_own, k_oth, v_oth, k_buf, v_buf, cos_ref, sin_ref, k_out, v_out, *, n_own):
    prompt = pl.program_id(0)
    local = prompt - pos_ref[0]
    is_own = (local >= 0) & (local < n_own)
    half, seq = cos_ref.shape
    valid = lax.broadcasted_iota(jnp.int32, (half, seq), 1) < len_ref[prompt]

    def emit(k_ref, v_ref):
        cos_t, sin_t = cos_ref[...], sin_ref[...]
        for h in range(k_out.shape[1]):
            first = k_ref[0, h, :half, :].astype(F32)
            second = k_ref[0, h, half:, :].astype(F32)
            lo, hi = rope_rows(first, second, cos_t, sin_t)
            k_out[0, h, :half, :] = jnp.where(valid, lo, k_buf[0, h, :half, :].astype(F32)).astype(BF16)
            k_out[0, h, half:, :] = jnp.where(valid, hi, k_buf[0, h, half:, :].astype(F32)).astype(BF16)
            for part in (slice(0, half), slice(half, 2 * half)):
                v_out[0, h, part, :] = jnp.where(valid, v_ref[0, h, part, :].astype(F32), v_buf[0, h, part, :].astype(F32)).astype(BF16)

    @pl.when(is_own)
    def _():
        emit(k_own, v_own)

    @pl.when(jnp.logical_not(is_own))
    def _():
        emit(k_oth, v_oth)


def fill_cache(pos, lengths, k_own, v_own, k_oth, v_oth, k_buf, v_buf, angles):
    batch, heads, hd, seq = k_buf.shape
    n_own, n_oth = k_own.shape[0], k_oth.shape[0]
    blk = 8
    steps = heads // blk

    def own_map(p, j, pos, _):
        local = p - pos[0]
        inside = (local >= 0) & (local < n_own)
        return (jnp.clip(local, 0, n_own - 1), pos[2] * steps + jnp.where(inside, j, jnp.where(local < 0, 0, steps - 1)), 0, 0)

    def oth_map(p, j, pos, _):
        local = p - pos[1]
        inside = (local >= 0) & (local < n_oth)
        return (jnp.clip(local, 0, n_oth - 1), jnp.where(inside, j, jnp.where(local < 0, 0, steps - 1)), 0, 0)

    shape = (1, blk, hd, seq)
    plain = pl.BlockSpec(shape, lambda p, j, *_: (p, j, 0, 0))
    table = pl.BlockSpec((hd // 2, seq), lambda p, j, *_: (0, 0))
    out = jax.ShapeDtypeStruct(k_buf.shape, BF16)
    return pl.pallas_call(
        functools.partial(cache_kernel, n_own=n_own),
        grid_spec=pltpu.PrefetchScalarGridSpec(
            num_scalar_prefetch=2,
            grid=(batch, steps),
            in_specs=[pl.BlockSpec(shape, own_map), pl.BlockSpec(shape, own_map), pl.BlockSpec(shape, oth_map), pl.BlockSpec(shape, oth_map), plain, plain, table, table],
            out_specs=[plain, plain],
        ),
        out_shape=[out, out],
        compiler_params=pltpu.CompilerParams(dimension_semantics=("arbitrary", "arbitrary")),
        cost_estimate=pl.CostEstimate(flops=40 * 10**9, bytes_accessed=12 * k_buf.size, transcendentals=0),
        name="fill_cache",
    )(pos, lengths, k_own, v_own, k_oth, v_oth, k_buf, v_buf, jnp.cos(angles).T, jnp.sin(angles).T)


def unpack_qkv(w_qkv, head_dim):
    cols = w_qkv.shape[1]
    third = cols // 3
    out_col = jnp.arange(cols)
    kind, rest = out_col // third, out_col % third
    source = (rest // head_dim) * 3 * head_dim + kind * head_dim + rest % head_dim
    select = (jnp.arange(cols)[:, None] == source[None, :]).astype(BF16)
    plain = jnp.dot(w_qkv, select, preferred_element_type=F32).astype(BF16)
    return plain[:, :third], plain[:, third:2 * third], plain[:, 2 * third:]


def solution(mesh):
    n_tpa = mesh.shape['tpa']

    def local_step(x_loc, len_loc, k_buf, v_buf, w_qkv, w_o, w_gate_up, w_down, g_attn, g_mlp):
        batch, seq, _ = x_loc.shape
        heads, head_dim = k_buf.shape[2:]
        n_oth = batch // n_tpa - SHARED // 2
        n_own = batch - n_oth
        mine = lax.axis_index('tpa')
        own_at, oth_at = mine * n_oth, (1 - mine) * n_own
        axes = ('tpa', 'tpb')
        take = lambda arr, at, n, axis=0: lax.dynamic_slice_in_dim(arr, at, n, axis)
        cols = lambda w: lax.all_gather(w, axes, axis=1, tiled=True)
        rows = lambda w: lax.all_gather(w, axes, axis=0, tiled=True)

        wq, wk, wv = unpack_qkv(w_qkv, head_dim)
        ff = w_gate_up.shape[1] // 2
        wk, wv, wq = cols(wk), cols(wv), cols(wq)
        wo = rows(w_o)
        wgate, wup = cols(w_gate_up[:, :ff]), cols(w_gate_up[:, ff:])
        wdown = rows(w_down)
        share = lambda w, axis: take(w, mine * (w.shape[axis] // n_tpa), w.shape[axis] // n_tpa, axis)
        out_w = (share(wq, 1), share(wk, 1), share(wv, 1), share(wo, 0), share(wgate, 1), share(wup, 1), share(wdown, 0))

        angles = rope_angles(seq, head_dim)
        u = rms_norm(x_loc, g_attn)
        x_own, u_own, u_oth = take(x_loc, own_at, n_own), take(u, own_at, n_own), take(u, oth_at, n_oth)
        len_own = take(len_loc, own_at, n_own)
        k_t, v_t = matmul_t(u_own, wk), matmul_t(u_own, wv)
        q = matmul(u_own, wq).astype(BF16)
        k_oth, v_oth = matmul_t(u_oth, out_w[1]), matmul_t(u_oth, out_w[2])
        attn = attention(len_own, q, k_t, v_t, angles)
        hidden = (x_own.astype(F32) + matmul(attn, wo)).astype(BF16)
        u2 = rms_norm(hidden, g_mlp)
        gate = matmul(u2, wgate).astype(BF16)
        up = matmul(u2, wup).astype(BF16)
        mid = (jax.nn.silu(gate.astype(F32)) * up.astype(F32)).astype(BF16)

        heads_of = lambda t: t.reshape(t.shape[0], t.shape[1] // head_dim, head_dim, seq)
        turn = lambda t: jnp.transpose(t, (0, 2, 3, 1))
        pos = jnp.stack([own_at, oth_at, mine]).astype(jnp.int32)
        k_cache, v_cache = fill_cache(pos, len_loc, heads_of(k_t), heads_of(v_t), heads_of(k_oth), heads_of(v_oth), turn(k_buf), turn(v_buf), angles)
        back = lambda t: jnp.transpose(t, (0, 3, 1, 2))

        swap = [(i, n_tpa - 1 - i) for i in range(n_tpa)]
        y_out = jnp.zeros(x_loc.shape, BF16)
        sent_at = mine * (n_own - n_oth)
        for start in range(0, n_oth, CHUNK):
            n = min(CHUNK, n_oth - start)
            local = sent_at + start
            part = (take(hidden, local, n).astype(F32) + matmul(take(mid, local, n), wdown)).astype(BF16)
            other = lax.ppermute(part, 'tpa', swap)
            y_out = lax.dynamic_update_slice_in_dim(y_out, part, own_at + local, 0)
            y_out = lax.dynamic_update_slice_in_dim(y_out, other, oth_at + start, 0)
        return (y_out, back(k_cache), back(v_cache)) + out_w

    batch_spec = P(('part', 'tpb'), None, None)
    len_spec = P(('part', 'tpb'))
    cache_spec = P(('part', 'tpb'), None, 'tpa', None)
    train_cols = P('part', ('tpa', 'tpb'))
    train_rows = P(('part', 'tpa', 'tpb'), None)
    gain_spec = P('part')
    gen_cols = P('part', 'tpa')
    gen_rows = P(('part', 'tpa'), None)
    return jax.shard_map(local_step, mesh=mesh, in_specs=(batch_spec, len_spec, cache_spec, cache_spec, train_cols, train_rows, train_cols, train_rows, gain_spec, gain_spec), out_specs=(batch_spec, cache_spec, cache_spec, gen_cols, gen_cols, gen_cols, gen_rows, gen_cols, gen_cols, gen_rows), check_vma=False)
```

```python
import functools
import math
import jax
import jax.numpy as jnp
from jax import lax
from jax.experimental import pallas as pl
from jax.experimental.layout import Layout, with_layout_constraint
from jax.experimental.pallas import tpu as pltpu
from jax.sharding import PartitionSpec as P


ROPE_BASE = 500000.0
ROPE_FACTOR = 8.0
LOW_FREQ = 1.0
HIGH_FREQ = 4.0
ORIG_CONTEXT = 8192.0
NORM_EPS = 1e-5
MASK_VALUE = -1e30
BF16 = jnp.bfloat16
F32 = jnp.float32
SHARED = 0
CHUNKS = (1, 1, 2, 2, 2)


def rms_norm(x_in, gain_vec):
    x_wide = x_in.astype(F32)
    mean_sq = jnp.mean(x_wide * x_wide, axis=-1, keepdims=True)
    return (x_wide * lax.rsqrt(mean_sq + NORM_EPS) * gain_vec.astype(F32)).astype(BF16)


def rope_angles(seq_len, head_dim):
    exponent = jnp.arange(head_dim // 2, dtype=F32) * (2.0 / head_dim)
    inv_freq = 1.0 / jnp.power(ROPE_BASE, exponent)
    wavelen = 2.0 * math.pi / inv_freq
    smooth = (ORIG_CONTEXT / wavelen - LOW_FREQ) / (HIGH_FREQ - LOW_FREQ)
    blended = (1.0 - smooth) * inv_freq / ROPE_FACTOR + smooth * inv_freq
    freq = jnp.where(wavelen < ORIG_CONTEXT / HIGH_FREQ, inv_freq, jnp.where(wavelen > ORIG_CONTEXT / LOW_FREQ, inv_freq / ROPE_FACTOR, blended))
    return jnp.arange(seq_len, dtype=F32)[:, None] * freq[None, :]


def matmul(lhs, rhs):
    return jnp.einsum('bsd,dc->bsc', lhs, rhs, preferred_element_type=F32)


def matmul_t(lhs, rhs):
    prod = with_layout_constraint(matmul(lhs, rhs), Layout((0, 2, 1)))
    return jnp.transpose(prod, (0, 2, 1)).astype(BF16)


def rope_rows(first, second, cos_t, sin_t):
    return first * cos_t - second * sin_t, second * cos_t + first * sin_t


def attn_kernel(len_ref, q_ref, k_ref, v_ref, cos_ref, sin_ref, cos_t_ref, sin_t_ref, o_ref, *, half, blk):
    seq = q_ref.shape[1]
    hd = 2 * half
    pair = 2 * hd
    length = len_ref[pl.program_id(0)]
    cos_t, sin_t = cos_t_ref[...], sin_t_ref[...]
    lane = lax.broadcasted_iota(jnp.int32, (blk, pair), 1)
    blocks = range(seq // blk)
    masks = []
    for i in blocks:
        row = lax.broadcasted_iota(jnp.int32, (blk, (i + 1) * blk), 0) + i * blk
        col = lax.broadcasted_iota(jnp.int32, (blk, (i + 1) * blk), 1)
        masks.append(col <= jnp.minimum(row, length - 1))
    for p in range(q_ref.shape[2] // pair):
        cols = slice(p * pair, (p + 1) * pair)
        keys = []
        for h in range(2):
            at = p * pair + h * hd
            keys += rope_rows(k_ref[0, at:at + half, :].astype(F32), k_ref[0, at + half:at + hd, :].astype(F32), cos_t, sin_t)
        keys = jnp.concatenate([part.astype(BF16) for part in keys], axis=0)
        scores = {}
        for i in blocks:
            rows = slice(i * blk, (i + 1) * blk)
            q_in = q_ref[0, rows, cols].astype(F32)
            swapped = jnp.where(lane % hd < half, pltpu.roll(q_in, pair - half, 1), pltpu.roll(q_in, half, 1))
            q_rot = (q_in * cos_ref[rows, :] + swapped * sin_ref[rows, :]).astype(BF16) * BF16(hd ** -0.5)
            for h in range(2):
                q_head = jnp.where(lane // hd == h, q_rot, BF16(0))
                scores[i, h] = jnp.dot(q_head, keys[:, :(i + 1) * blk], preferred_element_type=F32)
        tops = {}
        for i, h in scores:
            scores[i, h] = jnp.where(masks[i], scores[i, h], MASK_VALUE)
            tops[i, h] = jnp.max(scores[i, h], axis=-1, keepdims=True)
        values = v_ref[0, cols, :]
        outs = {}
        for i, h in scores:
            expd = jnp.exp(scores[i, h] - tops[i, h])
            norm = 1.0 / jnp.sum(expd, axis=-1, keepdims=True)
            out = lax.dot_general(expd.astype(BF16), values[:, :(i + 1) * blk], (((1,), (1,)), ((), ())), preferred_element_type=F32)
            outs[i, h] = out * norm
        for i in blocks:
            o_ref[0, i * blk:(i + 1) * blk, cols] = jnp.where(lane < hd, outs[i, 0], outs[i, 1]).astype(BF16)


def attention(lengths, q, k_t, v_t, angles):
    batch, seq, width = q.shape
    half = angles.shape[1]
    hd = 2 * half
    cos, sin = jnp.cos(angles), jnp.sin(angles)
    cos_row = jnp.tile(jnp.concatenate([cos, cos], axis=1), (1, 2))
    sin_row = jnp.tile(jnp.concatenate([-sin, sin], axis=1), (1, 2))
    whole = lambda shape: pl.BlockSpec(shape, lambda b, j, *_: (0, 0))
    group = 4 * hd
    return pl.pallas_call(
        functools.partial(attn_kernel, half=half, blk=256),
        grid_spec=pltpu.PrefetchScalarGridSpec(
            num_scalar_prefetch=1,
            grid=(batch, width // group),
            in_specs=[
                pl.BlockSpec((1, seq, group), lambda b, j, *_: (b, 0, j)),
                pl.BlockSpec((1, group, seq), lambda b, j, *_: (b, j, 0)),
                pl.BlockSpec((1, group, seq), lambda b, j, *_: (b, j, 0)),
                whole((seq, 2 * hd)), whole((seq, 2 * hd)), whole((half, seq)), whole((half, seq)),
            ],
            out_specs=pl.BlockSpec((1, seq, group), lambda b, j, *_: (b, 0, j)),
        ),
        out_shape=jax.ShapeDtypeStruct(q.shape, BF16),
        compiler_params=pltpu.CompilerParams(dimension_semantics=("parallel", "arbitrary")),
        cost_estimate=pl.CostEstimate(flops=batch * width * seq * seq * 16, bytes_accessed=8 * q.size, transcendentals=0),
        name="prefill_attention",
    )(lengths, q, k_t, v_t, cos_row, sin_row, cos.T, sin.T)


def cache_kernel(pos_ref, len_ref, k_own, v_own, k_oth, v_oth, k_buf, v_buf, cos_ref, sin_ref, k_out, v_out, *, n_own):
    prompt = pl.program_id(0)
    local = prompt - pos_ref[0]
    is_own = (local >= 0) & (local < n_own)
    half, seq = cos_ref.shape
    valid = lax.broadcasted_iota(jnp.int32, (half, seq), 1) < len_ref[prompt]

    def emit(k_ref, v_ref):
        cos_t, sin_t = cos_ref[...], sin_ref[...]
        for h in range(k_out.shape[1]):
            first = k_ref[0, h, :half, :].astype(F32)
            second = k_ref[0, h, half:, :].astype(F32)
            lo, hi = rope_rows(first, second, cos_t, sin_t)
            k_out[0, h, :half, :] = jnp.where(valid, lo, k_buf[0, h, :half, :].astype(F32)).astype(BF16)
            k_out[0, h, half:, :] = jnp.where(valid, hi, k_buf[0, h, half:, :].astype(F32)).astype(BF16)
            for part in (slice(0, half), slice(half, 2 * half)):
                v_out[0, h, part, :] = jnp.where(valid, v_ref[0, h, part, :].astype(F32), v_buf[0, h, part, :].astype(F32)).astype(BF16)

    @pl.when(is_own)
    def _():
        emit(k_own, v_own)

    @pl.when(jnp.logical_not(is_own))
    def _():
        emit(k_oth, v_oth)


def fill_cache(pos, lengths, k_own, v_own, k_oth, v_oth, k_buf, v_buf, angles):
    batch, heads, hd, seq = k_buf.shape
    n_own, n_oth = k_own.shape[0], k_oth.shape[0]
    blk = 8
    steps = heads // blk

    def own_map(p, j, pos, _):
        local = p - pos[0]
        inside = (local >= 0) & (local < n_own)
        return (jnp.clip(local, 0, n_own - 1), pos[2] * steps + jnp.where(inside, j, jnp.where(local < 0, 0, steps - 1)), 0, 0)

    def oth_map(p, j, pos, _):
        local = p - pos[1]
        inside = (local >= 0) & (local < n_oth)
        return (jnp.clip(local, 0, n_oth - 1), jnp.where(inside, j, jnp.where(local < 0, 0, steps - 1)), 0, 0)

    shape = (1, blk, hd, seq)
    plain = pl.BlockSpec(shape, lambda p, j, *_: (p, j, 0, 0))
    table = pl.BlockSpec((hd // 2, seq), lambda p, j, *_: (0, 0))
    out = jax.ShapeDtypeStruct(k_buf.shape, BF16)
    return pl.pallas_call(
        functools.partial(cache_kernel, n_own=n_own),
        grid_spec=pltpu.PrefetchScalarGridSpec(
            num_scalar_prefetch=2,
            grid=(batch, steps),
            in_specs=[pl.BlockSpec(shape, own_map), pl.BlockSpec(shape, own_map), pl.BlockSpec(shape, oth_map), pl.BlockSpec(shape, oth_map), plain, plain, table, table],
            out_specs=[plain, plain],
        ),
        out_shape=[out, out],
        compiler_params=pltpu.CompilerParams(dimension_semantics=("arbitrary", "arbitrary")),
        cost_estimate=pl.CostEstimate(flops=40 * 10**9, bytes_accessed=12 * k_buf.size, transcendentals=0),
        name="fill_cache",
    )(pos, lengths, k_own, v_own, k_oth, v_oth, k_buf, v_buf, jnp.cos(angles).T, jnp.sin(angles).T)


def unpack_qkv(w_qkv, head_dim):
    cols = w_qkv.shape[1]
    third = cols // 3
    out_col = jnp.arange(cols)
    kind, rest = out_col // third, out_col % third
    source = (rest // head_dim) * 3 * head_dim + kind * head_dim + rest % head_dim
    select = (jnp.arange(cols)[:, None] == source[None, :]).astype(BF16)
    plain = jnp.dot(w_qkv, select, preferred_element_type=F32).astype(BF16)
    return [with_layout_constraint(plain[:, k * third:(k + 1) * third], Layout((0, 1))) for k in range(3)]


def solution(mesh):
    n_tpa = mesh.shape['tpa']

    def local_step(x_loc, len_loc, k_buf, v_buf, w_qkv, w_o, w_gate_up, w_down, g_attn, g_mlp):
        batch, seq, _ = x_loc.shape
        _, head_dim = k_buf.shape[2:]
        n_oth = batch // n_tpa - SHARED // 2
        n_own = batch - n_oth
        mine = lax.axis_index('tpa')
        own_at, oth_at = mine * n_oth, (1 - mine) * n_own
        axes = ('tpa', 'tpb')
        take = lambda arr, at, n, axis=0: lax.dynamic_slice_in_dim(arr, at, n, axis)
        cols = lambda w: with_layout_constraint(lax.all_gather(w, axes, axis=1, tiled=True), Layout((0, 1)))
        rows = lambda w: lax.all_gather(w, axes, axis=0, tiled=True)

        wq, wk, wv = unpack_qkv(w_qkv, head_dim)
        ff = w_gate_up.shape[1] // 2
        wk = cols(wk)
        wv = cols(wv)
        wq = cols(wq)
        wo = rows(w_o)
        wgate = cols(w_gate_up[:, :ff])
        wup = cols(w_gate_up[:, ff:])
        wdown = rows(w_down)
        share = lambda w, axis: take(w, mine * (w.shape[axis] // n_tpa), w.shape[axis] // n_tpa, axis)
        out_w = (share(wq, 1), share(wk, 1), share(wv, 1), share(wo, 0), share(wgate, 1), share(wup, 1), share(wdown, 0))

        angles = rope_angles(seq, head_dim)
        u = rms_norm(x_loc, g_attn)
        x_own, u_own, u_oth = take(x_loc, own_at, n_own), take(u, own_at, n_own), take(u, oth_at, n_oth)
        len_own = take(len_loc, own_at, n_own)
        k_t, v_t = matmul_t(u_own, wk), matmul_t(u_own, wv)
        q = matmul(u_own, wq).astype(BF16)
        k_oth = matmul_t(u_oth, out_w[1])
        v_oth = matmul_t(u_oth, out_w[2])
        attn = attention(len_own, q, k_t, v_t, angles)
        hidden = (x_own.astype(F32) + matmul(attn, wo)).astype(BF16)
        u2 = rms_norm(hidden, g_mlp)
        gate = matmul(u2, wgate).astype(BF16)
        up = matmul(u2, wup).astype(BF16)
        mid = (jax.nn.silu(gate.astype(F32)) * up.astype(F32)).astype(BF16)

        heads_of = lambda t: t.reshape(t.shape[0], t.shape[1] // head_dim, head_dim, seq)
        turn = lambda t: jnp.transpose(t, (0, 2, 3, 1))
        pos = jnp.stack([own_at, oth_at, mine]).astype(jnp.int32)
        k_cache, v_cache = fill_cache(pos, len_loc, heads_of(k_t), heads_of(v_t), heads_of(k_oth), heads_of(v_oth), turn(k_buf), turn(v_buf), angles)
        back = lambda t: jnp.transpose(t, (0, 3, 1, 2))

        swap = [(i, n_tpa - 1 - i) for i in range(n_tpa)]
        sent_at = mine * (n_own - n_oth)
        parts = []
        at = 0
        for n in CHUNKS:
            local = sent_at + at
            part = (take(hidden, local, n).astype(F32) + matmul(take(mid, local, n), wdown)).astype(BF16)
            other = lax.ppermute(part, 'tpa', swap)
            parts.append((at, local, part, other))
            at += n
        assert at == n_oth
        y_out = jnp.zeros(x_loc.shape, BF16)
        for at, local, part, _ in parts:
            y_out = lax.dynamic_update_slice_in_dim(y_out, part, own_at + local, 0)
        for at, local, _, other in parts:
            y_out = lax.dynamic_update_slice_in_dim(y_out, other, oth_at + at, 0)
        return (y_out, back(k_cache), back(v_cache)) + out_w

    batch_spec = P(('part', 'tpb'), None, None)
    len_spec = P(('part', 'tpb'))
    cache_spec = P(('part', 'tpb'), None, 'tpa', None)
    train_cols = P('part', ('tpa', 'tpb'))
    train_rows = P(('part', 'tpa', 'tpb'), None)
    gain_spec = P('part')
    gen_cols = P('part', 'tpa')
    gen_rows = P(('part', 'tpa'), None)

    return jax.shard_map(local_step, mesh=mesh, in_specs=(batch_spec, len_spec, cache_spec, cache_spec, train_cols, train_rows, train_cols, train_rows, gain_spec, gain_spec), out_specs=(batch_spec, cache_spec, cache_spec, gen_cols, gen_cols, gen_cols, gen_rows, gen_cols, gen_cols, gen_rows), check_vma=False)
```

```python
import functools
import math
import jax
import jax.numpy as jnp
from jax import lax
from jax.experimental import pallas as pl
from jax.experimental.layout import Layout, with_layout_constraint
from jax.experimental.pallas import tpu as pltpu
from jax.sharding import PartitionSpec as P


ROPE_BASE = 500000.0
ROPE_FACTOR = 8.0
LOW_FREQ = 1.0
HIGH_FREQ = 4.0
ORIG_CONTEXT = 8192.0
NORM_EPS = 1e-5
MASK_VALUE = -1e30
BF16 = jnp.bfloat16
F32 = jnp.float32
SHARED = 0
CHUNKS = (1, 2, 2, 2, 1)


def rms_norm(x_in, gain_vec):
    x_wide = x_in.astype(F32)
    mean_sq = jnp.mean(x_wide * x_wide, axis=-1, keepdims=True)
    return (x_wide * lax.rsqrt(mean_sq + NORM_EPS) * gain_vec.astype(F32)).astype(BF16)


def rope_angles(seq_len, head_dim):
    exponent = jnp.arange(head_dim // 2, dtype=F32) * (2.0 / head_dim)
    inv_freq = 1.0 / jnp.power(ROPE_BASE, exponent)
    wavelen = 2.0 * math.pi / inv_freq
    smooth = (ORIG_CONTEXT / wavelen - LOW_FREQ) / (HIGH_FREQ - LOW_FREQ)
    blended = (1.0 - smooth) * inv_freq / ROPE_FACTOR + smooth * inv_freq
    freq = jnp.where(wavelen < ORIG_CONTEXT / HIGH_FREQ, inv_freq, jnp.where(wavelen > ORIG_CONTEXT / LOW_FREQ, inv_freq / ROPE_FACTOR, blended))
    return jnp.arange(seq_len, dtype=F32)[:, None] * freq[None, :]


def matmul(lhs, rhs):
    return jnp.einsum('bsd,dc->bsc', lhs, rhs, preferred_element_type=F32)


def matmul_t(lhs, rhs):
    prod = with_layout_constraint(matmul(lhs, rhs), Layout((0, 2, 1)))
    return jnp.transpose(prod, (0, 2, 1)).astype(BF16)


def rope_rows(first, second, cos_t, sin_t):
    return first * cos_t - second * sin_t, second * cos_t + first * sin_t


def attn_kernel(len_ref, q_ref, k_ref, v_ref, cos_ref, sin_ref, cos_t_ref, sin_t_ref, o_ref, *, half, blk):
    seq = q_ref.shape[1]
    hd = 2 * half
    pair = 2 * hd
    length = len_ref[pl.program_id(0)]
    cos_t, sin_t = cos_t_ref[...], sin_t_ref[...]
    lane = lax.broadcasted_iota(jnp.int32, (blk, pair), 1)
    blocks = range(seq // blk)
    masks = []
    for i in blocks:
        row = lax.broadcasted_iota(jnp.int32, (blk, (i + 1) * blk), 0) + i * blk
        col = lax.broadcasted_iota(jnp.int32, (blk, (i + 1) * blk), 1)
        masks.append(col <= jnp.minimum(row, length - 1))
    for p in range(q_ref.shape[2] // pair):
        cols = slice(p * pair, (p + 1) * pair)
        keys = []
        for h in range(2):
            at = p * pair + h * hd
            keys += rope_rows(k_ref[0, at:at + half, :].astype(F32), k_ref[0, at + half:at + hd, :].astype(F32), cos_t, sin_t)
        keys = jnp.concatenate([part.astype(BF16) for part in keys], axis=0)
        scores = {}
        for i in blocks:
            rows = slice(i * blk, (i + 1) * blk)
            q_in = q_ref[0, rows, cols].astype(F32)
            swapped = jnp.where(lane % hd < half, pltpu.roll(q_in, pair - half, 1), pltpu.roll(q_in, half, 1))
            q_rot = (q_in * cos_ref[rows, :] + swapped * sin_ref[rows, :]).astype(BF16) * BF16(hd ** -0.5)
            for h in range(2):
                q_head = jnp.where(lane // hd == h, q_rot, BF16(0))
                scores[i, h] = jnp.dot(q_head, keys[:, :(i + 1) * blk], preferred_element_type=F32)
        tops = {}
        for i, h in scores:
            scores[i, h] = jnp.where(masks[i], scores[i, h], MASK_VALUE)
            tops[i, h] = jnp.max(scores[i, h], axis=-1, keepdims=True)
        values = v_ref[0, cols, :]
        outs = {}
        for i, h in scores:
            expd = jnp.exp(scores[i, h] - tops[i, h])
            norm = 1.0 / jnp.sum(expd, axis=-1, keepdims=True)
            out = lax.dot_general(expd.astype(BF16), values[:, :(i + 1) * blk], (((1,), (1,)), ((), ())), preferred_element_type=F32)
            outs[i, h] = out * norm
        for i in blocks:
            o_ref[0, i * blk:(i + 1) * blk, cols] = jnp.where(lane < hd, outs[i, 0], outs[i, 1]).astype(BF16)


def attention(lengths, q, k_t, v_t, angles):
    batch, seq, width = q.shape
    half = angles.shape[1]
    hd = 2 * half
    cos, sin = jnp.cos(angles), jnp.sin(angles)
    cos_row = jnp.tile(jnp.concatenate([cos, cos], axis=1), (1, 2))
    sin_row = jnp.tile(jnp.concatenate([-sin, sin], axis=1), (1, 2))
    whole = lambda shape: pl.BlockSpec(shape, lambda b, j, *_: (0, 0))
    group = 4 * hd
    return pl.pallas_call(
        functools.partial(attn_kernel, half=half, blk=256),
        grid_spec=pltpu.PrefetchScalarGridSpec(
            num_scalar_prefetch=1,
            grid=(batch, width // group),
            in_specs=[
                pl.BlockSpec((1, seq, group), lambda b, j, *_: (b, 0, j)),
                pl.BlockSpec((1, group, seq), lambda b, j, *_: (b, j, 0)),
                pl.BlockSpec((1, group, seq), lambda b, j, *_: (b, j, 0)),
                whole((seq, 2 * hd)), whole((seq, 2 * hd)), whole((half, seq)), whole((half, seq)),
            ],
            out_specs=pl.BlockSpec((1, seq, group), lambda b, j, *_: (b, 0, j)),
        ),
        out_shape=jax.ShapeDtypeStruct(q.shape, BF16),
        compiler_params=pltpu.CompilerParams(dimension_semantics=("parallel", "arbitrary")),
        cost_estimate=pl.CostEstimate(flops=batch * width * seq * seq * 16, bytes_accessed=8 * q.size, transcendentals=0),
        name="prefill_attention",
    )(lengths, q, k_t, v_t, cos_row, sin_row, cos.T, sin.T)


def cache_kernel(pos_ref, len_ref, k_own, v_own, k_oth, v_oth, k_buf, v_buf, cos_ref, sin_ref, k_out, v_out, *, n_own):
    prompt = pl.program_id(0)
    local = prompt - pos_ref[0]
    is_own = (local >= 0) & (local < n_own)
    half, seq = cos_ref.shape
    valid = lax.broadcasted_iota(jnp.int32, (half, seq), 1) < len_ref[prompt]

    def emit(k_ref, v_ref):
        cos_t, sin_t = cos_ref[...], sin_ref[...]
        for h in range(k_out.shape[1]):
            first = k_ref[0, h, :half, :].astype(F32)
            second = k_ref[0, h, half:, :].astype(F32)
            lo, hi = rope_rows(first, second, cos_t, sin_t)
            k_out[0, h, :half, :] = jnp.where(valid, lo, k_buf[0, h, :half, :].astype(F32)).astype(BF16)
            k_out[0, h, half:, :] = jnp.where(valid, hi, k_buf[0, h, half:, :].astype(F32)).astype(BF16)
            for part in (slice(0, half), slice(half, 2 * half)):
                v_out[0, h, part, :] = jnp.where(valid, v_ref[0, h, part, :].astype(F32), v_buf[0, h, part, :].astype(F32)).astype(BF16)

    @pl.when(is_own)
    def _():
        emit(k_own, v_own)

    @pl.when(jnp.logical_not(is_own))
    def _():
        emit(k_oth, v_oth)


def fill_cache(pos, lengths, k_own, v_own, k_oth, v_oth, k_buf, v_buf, angles):
    batch, heads, hd, seq = k_buf.shape
    n_own, n_oth = k_own.shape[0], k_oth.shape[0]
    blk = 8
    steps = heads // blk

    def own_map(p, j, pos, _):
        local = p - pos[0]
        inside = (local >= 0) & (local < n_own)
        return (jnp.clip(local, 0, n_own - 1), pos[2] * steps + jnp.where(inside, j, jnp.where(local < 0, 0, steps - 1)), 0, 0)

    def oth_map(p, j, pos, _):
        local = p - pos[1]
        inside = (local >= 0) & (local < n_oth)
        return (jnp.clip(local, 0, n_oth - 1), jnp.where(inside, j, jnp.where(local < 0, 0, steps - 1)), 0, 0)

    shape = (1, blk, hd, seq)
    plain = pl.BlockSpec(shape, lambda p, j, *_: (p, j, 0, 0))
    table = pl.BlockSpec((hd // 2, seq), lambda p, j, *_: (0, 0))
    out = jax.ShapeDtypeStruct(k_buf.shape, BF16)
    return pl.pallas_call(
        functools.partial(cache_kernel, n_own=n_own),
        grid_spec=pltpu.PrefetchScalarGridSpec(
            num_scalar_prefetch=2,
            grid=(batch, steps),
            in_specs=[pl.BlockSpec(shape, own_map), pl.BlockSpec(shape, own_map), pl.BlockSpec(shape, oth_map), pl.BlockSpec(shape, oth_map), plain, plain, table, table],
            out_specs=[plain, plain],
        ),
        out_shape=[out, out],
        compiler_params=pltpu.CompilerParams(dimension_semantics=("arbitrary", "arbitrary")),
        cost_estimate=pl.CostEstimate(flops=40 * 10**9, bytes_accessed=12 * k_buf.size, transcendentals=0),
        name="fill_cache",
    )(pos, lengths, k_own, v_own, k_oth, v_oth, k_buf, v_buf, jnp.cos(angles).T, jnp.sin(angles).T)


def unpack_qkv(w_qkv, head_dim):
    cols = w_qkv.shape[1]
    third = cols // 3
    out_col = jnp.arange(cols)
    kind, rest = out_col // third, out_col % third
    source = (rest // head_dim) * 3 * head_dim + kind * head_dim + rest % head_dim
    select = (jnp.arange(cols)[:, None] == source[None, :]).astype(BF16)
    plain = jnp.dot(w_qkv, select, preferred_element_type=F32).astype(BF16)
    return [with_layout_constraint(plain[:, k * third:(k + 1) * third], Layout((0, 1))) for k in range(3)]


def solution(mesh):
    n_tpa = mesh.shape['tpa']

    def local_step(x_loc, len_loc, k_buf, v_buf, w_qkv, w_o, w_gate_up, w_down, g_attn, g_mlp):
        batch, seq, _ = x_loc.shape
        _, head_dim = k_buf.shape[2:]
        n_oth = batch // n_tpa - SHARED // 2
        n_own = batch - n_oth
        mine = lax.axis_index('tpa')
        own_at, oth_at = mine * n_oth, (1 - mine) * n_own
        axes = ('tpa', 'tpb')
        take = lambda arr, at, n, axis=0: lax.dynamic_slice_in_dim(arr, at, n, axis)
        cols = lambda w: with_layout_constraint(lax.all_gather(w, axes, axis=1, tiled=True), Layout((0, 1)))
        rows = lambda w: lax.all_gather(w, axes, axis=0, tiled=True)

        wq, wk, wv = unpack_qkv(w_qkv, head_dim)
        ff = w_gate_up.shape[1] // 2
        wkv = with_layout_constraint(lax.all_gather(jnp.stack([wk, wv]), axes, axis=2, tiled=True), Layout((0, 1, 2)))
        wk, wv = wkv[0], wkv[1]
        wq = cols(wq)
        wo = rows(w_o)
        wgate = cols(w_gate_up[:, :ff])
        wup = cols(w_gate_up[:, ff:])
        wdown = rows(w_down)
        share = lambda w, axis: take(w, mine * (w.shape[axis] // n_tpa), w.shape[axis] // n_tpa, axis)
        n_cols = wkv.shape[2] // n_tpa
        part_of = lambda k: lax.dynamic_slice(wkv, (k, 0, mine * n_cols), (1, wkv.shape[1], n_cols))[0]
        out_w = (share(wq, 1), part_of(0), part_of(1), share(wo, 0), share(wgate, 1), share(wup, 1), share(wdown, 0))

        angles = rope_angles(seq, head_dim)
        u = rms_norm(x_loc, g_attn)
        x_own, u_own, u_oth = take(x_loc, own_at, n_own), take(u, own_at, n_own), take(u, oth_at, n_oth)
        len_own = take(len_loc, own_at, n_own)
        k_t, v_t = matmul_t(u_own, wk), matmul_t(u_own, wv)
        q = matmul(u_own, wq).astype(BF16)
        k_oth = matmul_t(u_oth, out_w[1])
        v_oth = matmul_t(u_oth, out_w[2])
        attn = attention(len_own, q, k_t, v_t, angles)
        hidden = (x_own.astype(F32) + matmul(attn, wo)).astype(BF16)
        u2 = rms_norm(hidden, g_mlp)
        gate = matmul(u2, wgate).astype(BF16)
        up = matmul(u2, wup).astype(BF16)
        mid = (jax.nn.silu(gate.astype(F32)) * up.astype(F32)).astype(BF16)

        heads_of = lambda t: t.reshape(t.shape[0], t.shape[1] // head_dim, head_dim, seq)
        turn = lambda t: jnp.transpose(t, (0, 2, 3, 1))
        pos = jnp.stack([own_at, oth_at, mine]).astype(jnp.int32)
        k_cache, v_cache = fill_cache(pos, len_loc, heads_of(k_t), heads_of(v_t), heads_of(k_oth), heads_of(v_oth), turn(k_buf), turn(v_buf), angles)
        back = lambda t: jnp.transpose(t, (0, 3, 1, 2))

        swap = [(i, n_tpa - 1 - i) for i in range(n_tpa)]
        sent_at = mine * (n_own - n_oth)
        parts = []
        at = 0
        for n in CHUNKS:
            local = sent_at + at
            part = (take(hidden, local, n).astype(F32) + matmul(take(mid, local, n), wdown)).astype(BF16)
            other = lax.ppermute(part, 'tpa', swap)
            parts.append((at, local, part, other))
            at += n
        assert at == n_oth
        y_out = jnp.zeros(x_loc.shape, BF16)
        for at, local, part, _ in parts:
            y_out = lax.dynamic_update_slice_in_dim(y_out, part, own_at + local, 0)
        for at, local, _, other in parts:
            y_out = lax.dynamic_update_slice_in_dim(y_out, other, oth_at + at, 0)
        return (y_out, back(k_cache), back(v_cache)) + out_w

    batch_spec = P(('part', 'tpb'), None, None)
    len_spec = P(('part', 'tpb'))
    cache_spec = P(('part', 'tpb'), None, 'tpa', None)
    train_cols = P('part', ('tpa', 'tpb'))
    train_rows = P(('part', 'tpa', 'tpb'), None)
    gain_spec = P('part')
    gen_cols = P('part', 'tpa')
    gen_rows = P(('part', 'tpa'), None)

    return jax.shard_map(local_step, mesh=mesh, in_specs=(batch_spec, len_spec, cache_spec, cache_spec, train_cols, train_rows, train_cols, train_rows, gain_spec, gain_spec), out_specs=(batch_spec, cache_spec, cache_spec, gen_cols, gen_cols, gen_cols, gen_rows, gen_cols, gen_cols, gen_rows), check_vma=False)
```

```python
import functools
import math
import jax
import jax.numpy as jnp
from jax import lax
from jax.experimental import pallas as pl
from jax.experimental.layout import Layout, with_layout_constraint
from jax.experimental.pallas import tpu as pltpu
from jax.sharding import PartitionSpec as P


ROPE_BASE = 500000.0
ROPE_FACTOR = 8.0
LOW_FREQ = 1.0
HIGH_FREQ = 4.0
ORIG_CONTEXT = 8192.0
NORM_EPS = 1e-5
MASK_VALUE = -1e30
BF16 = jnp.bfloat16
F32 = jnp.float32
CHUNKS = (1, 2, 2, 2, 1)


def rms_norm(x_in, gain_vec):
    x_wide = x_in.astype(F32)
    mean_sq = jnp.mean(x_wide * x_wide, axis=-1, keepdims=True)
    return (x_wide * lax.rsqrt(mean_sq + NORM_EPS) * gain_vec.astype(F32)).astype(BF16)


def rope_angles(seq_len, head_dim):
    exponent = jnp.arange(head_dim // 2, dtype=F32) * (2.0 / head_dim)
    inv_freq = 1.0 / jnp.power(ROPE_BASE, exponent)
    wavelen = 2.0 * math.pi / inv_freq
    smooth = (ORIG_CONTEXT / wavelen - LOW_FREQ) / (HIGH_FREQ - LOW_FREQ)
    blended = (1.0 - smooth) * inv_freq / ROPE_FACTOR + smooth * inv_freq
    freq = jnp.where(wavelen < ORIG_CONTEXT / HIGH_FREQ, inv_freq, jnp.where(wavelen > ORIG_CONTEXT / LOW_FREQ, inv_freq / ROPE_FACTOR, blended))
    return jnp.arange(seq_len, dtype=F32)[:, None] * freq[None, :]


def matmul(lhs, rhs):
    return jnp.einsum('bsd,dc->bsc', lhs, rhs, preferred_element_type=F32)


def matmul_t(lhs, rhs):
    prod = with_layout_constraint(matmul(lhs, rhs), Layout((0, 2, 1)))
    return jnp.transpose(prod, (0, 2, 1)).astype(BF16)


def rope_rows(first, second, cos_t, sin_t):
    return first * cos_t - second * sin_t, second * cos_t + first * sin_t


def attn_kernel(len_ref, q_ref, k_ref, v_ref, cos_ref, sin_ref, cos_t_ref, sin_t_ref, o_ref, *, half, blk):
    seq = q_ref.shape[1]
    hd = 2 * half
    pair = 2 * hd
    length = len_ref[pl.program_id(0)]
    cos_t, sin_t = cos_t_ref[...], sin_t_ref[...]
    lane = lax.broadcasted_iota(jnp.int32, (blk, pair), 1)
    blocks = range(seq // blk)
    masks = []
    for i in blocks:
        row = lax.broadcasted_iota(jnp.int32, (blk, (i + 1) * blk), 0) + i * blk
        col = lax.broadcasted_iota(jnp.int32, (blk, (i + 1) * blk), 1)
        masks.append(col <= jnp.minimum(row, length - 1))
    for p in range(q_ref.shape[2] // pair):
        cols = slice(p * pair, (p + 1) * pair)
        keys = []
        for h in range(2):
            at = p * pair + h * hd
            keys += rope_rows(k_ref[0, at:at + half, :].astype(F32), k_ref[0, at + half:at + hd, :].astype(F32), cos_t, sin_t)
        keys = jnp.concatenate([part.astype(BF16) for part in keys], axis=0)
        scores = {}
        for i in blocks:
            rows = slice(i * blk, (i + 1) * blk)
            q_in = q_ref[0, rows, cols].astype(F32)
            swapped = jnp.where(lane % hd < half, pltpu.roll(q_in, pair - half, 1), pltpu.roll(q_in, half, 1))
            q_rot = (q_in * cos_ref[rows, :] + swapped * sin_ref[rows, :]).astype(BF16) * BF16(hd ** -0.5)
            for h in range(2):
                q_head = jnp.where(lane // hd == h, q_rot, BF16(0))
                scores[i, h] = jnp.dot(q_head, keys[:, :(i + 1) * blk], preferred_element_type=F32)
        tops = {}
        for i, h in scores:
            scores[i, h] = jnp.where(masks[i], scores[i, h], MASK_VALUE)
            tops[i, h] = jnp.max(scores[i, h], axis=-1, keepdims=True)
        values = v_ref[0, cols, :]
        outs = {}
        for i, h in scores:
            expd = jnp.exp(scores[i, h] - tops[i, h])
            norm = 1.0 / jnp.sum(expd, axis=-1, keepdims=True)
            out = lax.dot_general(expd.astype(BF16), values[:, :(i + 1) * blk], (((1,), (1,)), ((), ())), preferred_element_type=F32)
            outs[i, h] = out * norm
        for i in blocks:
            o_ref[0, i * blk:(i + 1) * blk, cols] = jnp.where(lane < hd, outs[i, 0], outs[i, 1]).astype(BF16)


def attention(lengths, q, k_t, v_t, angles):
    batch, seq, width = q.shape
    half = angles.shape[1]
    hd = 2 * half
    cos, sin = jnp.cos(angles), jnp.sin(angles)
    cos_row = jnp.tile(jnp.concatenate([cos, cos], axis=1), (1, 2))
    sin_row = jnp.tile(jnp.concatenate([-sin, sin], axis=1), (1, 2))
    whole = lambda shape: pl.BlockSpec(shape, lambda b, j, *_: (0, 0))
    group = 4 * hd
    return pl.pallas_call(
        functools.partial(attn_kernel, half=half, blk=256),
        grid_spec=pltpu.PrefetchScalarGridSpec(
            num_scalar_prefetch=1,
            grid=(batch, width // group),
            in_specs=[
                pl.BlockSpec((1, seq, group), lambda b, j, *_: (b, 0, j)),
                pl.BlockSpec((1, group, seq), lambda b, j, *_: (b, j, 0)),
                pl.BlockSpec((1, group, seq), lambda b, j, *_: (b, j, 0)),
                whole((seq, 2 * hd)), whole((seq, 2 * hd)), whole((half, seq)), whole((half, seq)),
            ],
            out_specs=pl.BlockSpec((1, seq, group), lambda b, j, *_: (b, 0, j)),
        ),
        out_shape=jax.ShapeDtypeStruct(q.shape, BF16),
        compiler_params=pltpu.CompilerParams(dimension_semantics=("parallel", "arbitrary")),
        cost_estimate=pl.CostEstimate(flops=batch * width * seq * seq * 16, bytes_accessed=8 * q.size, transcendentals=0),
        name="prefill_attention",
    )(lengths, q, k_t, v_t, cos_row, sin_row, cos.T, sin.T)


def cache_kernel(pos_ref, len_ref, k_own, v_own, k_oth, v_oth, k_buf, v_buf, cos_ref, sin_ref, k_out, v_out, *, n_own):
    prompt = pl.program_id(0)
    local = prompt - pos_ref[0]
    is_own = (local >= 0) & (local < n_own)
    half, seq = cos_ref.shape
    valid = lax.broadcasted_iota(jnp.int32, (half, seq), 1) < len_ref[prompt]

    def emit(k_ref, v_ref):
        cos_t, sin_t = cos_ref[...], sin_ref[...]
        for h in range(k_out.shape[1]):
            first = k_ref[0, h, :half, :].astype(F32)
            second = k_ref[0, h, half:, :].astype(F32)
            lo, hi = rope_rows(first, second, cos_t, sin_t)
            k_out[0, h, :half, :] = jnp.where(valid, lo, k_buf[0, h, :half, :].astype(F32)).astype(BF16)
            k_out[0, h, half:, :] = jnp.where(valid, hi, k_buf[0, h, half:, :].astype(F32)).astype(BF16)
            for part in (slice(0, half), slice(half, 2 * half)):
                v_out[0, h, part, :] = jnp.where(valid, v_ref[0, h, part, :].astype(F32), v_buf[0, h, part, :].astype(F32)).astype(BF16)

    @pl.when(is_own)
    def _():
        emit(k_own, v_own)

    @pl.when(jnp.logical_not(is_own))
    def _():
        emit(k_oth, v_oth)


def fill_cache(pos, lengths, k_own, v_own, k_oth, v_oth, k_buf, v_buf, angles):
    batch, heads, hd, seq = k_buf.shape
    n_own, n_oth = k_own.shape[0], k_oth.shape[0]
    blk = 8
    steps = heads // blk

    def own_map(p, j, pos, _):
        local = p - pos[0]
        inside = (local >= 0) & (local < n_own)
        return (jnp.clip(local, 0, n_own - 1), pos[2] * steps + jnp.where(inside, j, jnp.where(local < 0, 0, steps - 1)), 0, 0)

    def oth_map(p, j, pos, _):
        local = p - pos[1]
        inside = (local >= 0) & (local < n_oth)
        return (jnp.clip(local, 0, n_oth - 1), jnp.where(inside, j, jnp.where(local < 0, 0, steps - 1)), 0, 0)

    shape = (1, blk, hd, seq)
    plain = pl.BlockSpec(shape, lambda p, j, *_: (p, j, 0, 0))
    table = pl.BlockSpec((hd // 2, seq), lambda p, j, *_: (0, 0))
    out = jax.ShapeDtypeStruct(k_buf.shape, BF16)
    return pl.pallas_call(
        functools.partial(cache_kernel, n_own=n_own),
        grid_spec=pltpu.PrefetchScalarGridSpec(
            num_scalar_prefetch=2,
            grid=(batch, steps),
            in_specs=[pl.BlockSpec(shape, own_map), pl.BlockSpec(shape, own_map), pl.BlockSpec(shape, oth_map), pl.BlockSpec(shape, oth_map), plain, plain, table, table],
            out_specs=[plain, plain],
        ),
        out_shape=[out, out],
        compiler_params=pltpu.CompilerParams(dimension_semantics=("arbitrary", "arbitrary")),
        cost_estimate=pl.CostEstimate(flops=40 * 10**9, bytes_accessed=12 * k_buf.size, transcendentals=0),
        name="fill_cache",
    )(pos, lengths, k_own, v_own, k_oth, v_oth, k_buf, v_buf, jnp.cos(angles).T, jnp.sin(angles).T)


def unpack_qkv(w_qkv, head_dim):
    cols = w_qkv.shape[1]
    third = cols // 3
    out_col = jnp.arange(cols)
    kind, rest = out_col // third, out_col % third
    source = (rest // head_dim) * 3 * head_dim + kind * head_dim + rest % head_dim
    select = (jnp.arange(cols)[:, None] == source[None, :]).astype(BF16)
    plain = jnp.dot(w_qkv, select, preferred_element_type=F32).astype(BF16)
    return [with_layout_constraint(plain[:, k * third:(k + 1) * third], Layout((0, 1))) for k in range(3)]


def solution(mesh):
    n_tpa = mesh.shape['tpa']

    def local_step(x_loc, len_loc, k_buf, v_buf, w_qkv, w_o, w_gate_up, w_down, g_attn, g_mlp):
        batch, seq, _ = x_loc.shape
        _, head_dim = k_buf.shape[2:]
        n_own = n_oth = batch // n_tpa
        mine = lax.axis_index('tpa')
        own_at, oth_at = mine * n_oth, (1 - mine) * n_own
        axes = ('tpa', 'tpb')
        take = lambda arr, at, n, axis=0: lax.dynamic_slice_in_dim(arr, at, n, axis)
        cols = lambda w: with_layout_constraint(lax.all_gather(w, axes, axis=1, tiled=True), Layout((0, 1)))
        rows = lambda w: lax.all_gather(w, axes, axis=0, tiled=True)

        wq, wk, wv = unpack_qkv(w_qkv, head_dim)
        ff = w_gate_up.shape[1] // 2
        wkv = with_layout_constraint(lax.all_gather(jnp.stack([wk, wv]), axes, axis=2, tiled=True), Layout((0, 1, 2)))
        wk, wv = wkv[0], wkv[1]
        wq = cols(wq)
        wo = rows(w_o)
        wgate = cols(w_gate_up[:, :ff])
        wup = cols(w_gate_up[:, ff:])
        wdown = rows(w_down)
        share = lambda w, axis: take(w, mine * (w.shape[axis] // n_tpa), w.shape[axis] // n_tpa, axis)
        n_cols = wkv.shape[2] // n_tpa
        part_of = lambda k: lax.dynamic_slice(wkv, (k, 0, mine * n_cols), (1, wkv.shape[1], n_cols))[0]
        out_w = (share(wq, 1), part_of(0), part_of(1), share(wo, 0), share(wgate, 1), share(wup, 1), share(wdown, 0))

        angles = rope_angles(seq, head_dim)
        u = rms_norm(x_loc, g_attn)
        x_own, u_own, u_oth = take(x_loc, own_at, n_own), take(u, own_at, n_own), take(u, oth_at, n_oth)
        len_own = take(len_loc, own_at, n_own)
        k_t, v_t = matmul_t(u_own, wk), matmul_t(u_own, wv)
        q = matmul(u_own, wq).astype(BF16)
        k_oth = matmul_t(u_oth, out_w[1])
        v_oth = matmul_t(u_oth, out_w[2])
        attn = attention(len_own, q, k_t, v_t, angles)
        hidden = (x_own.astype(F32) + matmul(attn, wo)).astype(BF16)
        u2 = rms_norm(hidden, g_mlp)
        gate = matmul(u2, wgate).astype(BF16)
        glu = lambda lo, hi: (jax.nn.silu(gate[lo:hi].astype(F32)) * matmul(u2[lo:hi], wup).astype(BF16).astype(F32)).astype(BF16)
        late_at = n_own - CHUNKS[-1]
        mid_first = glu(0, late_at)
        mid_late = glu(late_at, n_own)

        heads_of = lambda t: t.reshape(t.shape[0], t.shape[1] // head_dim, head_dim, seq)
        turn = lambda t: jnp.transpose(t, (0, 2, 3, 1))
        pos = jnp.stack([own_at, oth_at, mine]).astype(jnp.int32)
        k_cache, v_cache = fill_cache(pos, len_loc, heads_of(k_t), heads_of(v_t), heads_of(k_oth), heads_of(v_oth), turn(k_buf), turn(v_buf), angles)
        back = lambda t: jnp.transpose(t, (0, 3, 1, 2))

        swap = [(i, n_tpa - 1 - i) for i in range(n_tpa)]
        parts = []
        at = 0
        for n in CHUNKS:
            mid = mid_late if at == late_at else mid_first[at:at + n]
            part = (hidden[at:at + n].astype(F32) + matmul(mid, wdown)).astype(BF16)
            other = lax.ppermute(part, 'tpa', swap)
            parts.append((at, part, other))
            at += n
        assert at == n_oth
        y_out = jnp.zeros(x_loc.shape, BF16)
        for at, part, _ in parts:
            y_out = lax.dynamic_update_slice_in_dim(y_out, part, own_at + at, 0)
        for at, _, other in parts:
            y_out = lax.dynamic_update_slice_in_dim(y_out, other, oth_at + at, 0)
        return (y_out, back(k_cache), back(v_cache)) + out_w

    batch_spec = P(('part', 'tpb'), None, None)
    len_spec = P(('part', 'tpb'))
    cache_spec = P(('part', 'tpb'), None, 'tpa', None)
    train_cols = P('part', ('tpa', 'tpb'))
    train_rows = P(('part', 'tpa', 'tpb'), None)
    gain_spec = P('part')
    gen_cols = P('part', 'tpa')
    gen_rows = P(('part', 'tpa'), None)

    return jax.shard_map(local_step, mesh=mesh, in_specs=(batch_spec, len_spec, cache_spec, cache_spec, train_cols, train_rows, train_cols, train_rows, gain_spec, gain_spec), out_specs=(batch_spec, cache_spec, cache_spec, gen_cols, gen_cols, gen_cols, gen_rows, gen_cols, gen_cols, gen_rows), check_vma=False)
```
